256 devices in a mesh: parts: 2 (over z), tok: 64 (over x, y), sub: 2 (over core).
Axes of the slice: x: 8, y: 8, z: 2, core: 2. Of those that a mesh axis runs over, the one named last changes fastest.
The devices are a block of a 8x8x16 slice.
Arguments:
- video: bfloat16 [16, 48, 128, 768], P('parts', None, ('tok', 'sub')), parts along dimension 0, may hold values from -6 to 6
- norm_gain: float32 [3, 768], replicated, may hold values from 0.1 to 1.9
- qkv_weight: bfloat16 [3, 3, 768, 768], P(None, None, None, 'sub'), may hold values from -0.21875 to 0.21875
- out_weight: bfloat16 [3, 768, 768], P(None, 'sub'), may hold values from -0.21875 to 0.21875
Outputs:
- refined: bfloat16 [16, 48, 128, 768], P('parts', None, ('tok', 'sub')), parts along dimension 0
The draws below stay inside these ranges and needn't reach their ends.
There are 2 independent parts, one for each index of `parts`. The reference program is written for one: setup_inputs(seed, part) draws one part's arguments, and reference() takes and returns one part's arrays. A program takes and returns all parts, laid end to end along the dimension named above; an argument that names none is the same for every part. Nothing has to cross between parts.
All inputs are finite; a program needn't handle non-finite values.
Results may differ from the reference program's by a relative error of at most 0.014.
Values may be sent and summed in bfloat16 or wider, within the bound.
A program may use at most 64 MiB of HBM per device.

```python
import math
import jax
import jax.numpy as jnp
from jax import lax

D = 768
HEAD_DIM = 64
T_SIZE = 8
H = 48
W = 128


def levels(rng, extent, shards, least, high):
    loudness, own = 1.0, jax.random.fold_in(rng, 6)
    for position, parts in shards:
        draws = jnp.exp(jax.random.uniform(jax.random.fold_in(own, position), (parts,), jnp.float32, least / len(shards), high / len(shards)))
        loudness = loudness * jnp.repeat(draws, extent[position] // parts).reshape([-1 if axis == position else 1 for axis in range(len(extent))])
    return loudness


def normal_values(key, extent, scale, reach, shards=(), held_as=jnp.bfloat16):
    loudness = levels(key, extent, shards, -0.22, 0.18) if shards else 1.0
    result = jax.random.normal(key, extent, jnp.float32) * scale * loudness
    return jnp.minimum(jnp.maximum(result, -reach), reach).astype(held_as)


def setup_inputs(seed: int = 0, part: int = 0) -> dict:
    splits = jax.random.split(jax.random.key(seed), 5)
    part_keys = jax.random.split(jax.random.fold_in(splits[4], part), 5)
    return {
        "video": normal_values(part_keys[0], (T_SIZE, H, W, D), 1.0, 6.0, ((2, 128),)),
        "norm_gain": jnp.clip(1.0 + 0.18 * jax.random.normal(splits[1], (3, D), jnp.float32), 0.1, 1.9),
        "qkv_weight": normal_values(splits[2], (3, 3, D, D), D ** -0.5, 0.21875, ((3, 2),)),
        "out_weight": normal_values(splits[3], (3, D, D), D ** -0.5, 0.21875, ((1, 2),)),
    }


EPSILON = 1e-06

def normalize(tokens, gain):
    values = tokens.astype(jnp.float32)
    scale = lax.rsqrt(lax.optimization_barrier(jnp.mean(values * values, axis=-1, keepdims=True)) + EPSILON)
    return (values * scale * gain.astype(jnp.float32)).astype(jnp.bfloat16)

def head_norm(values, shape):
    split = values.reshape(shape + (values.shape[-1] // HEAD_DIM, HEAD_DIM))
    scale = lax.rsqrt(lax.optimization_barrier(jnp.mean(split * split, axis=-1, keepdims=True)) + EPSILON)
    return (split * scale).astype(jnp.bfloat16)

def attend(query, key, value, shape):
    query_n = head_norm(query, shape)
    key_n = head_norm(key, shape)
    value_b = value.reshape(query_n.shape).astype(jnp.bfloat16)
    scores = jnp.einsum('plqhe,pmqhe->pqhlm', query_n.astype(jnp.float32), key_n.astype(jnp.float32)) / math.sqrt(HEAD_DIM)
    expo = jnp.exp(scores)
    probs = (expo / lax.optimization_barrier(jnp.sum(expo, axis=-1, keepdims=True))).astype(jnp.bfloat16)
    mixed = jnp.einsum('pqhlm,pmqhe->plqhe', probs.astype(jnp.float32), value_b.astype(jnp.float32))
    return mixed.astype(jnp.bfloat16).reshape(query.shape)

def sublayer(tokens, gain, qkv_part, out_part):
    shape = tokens.shape[:3]
    width = tokens.shape[3]
    flat = normalize(tokens, gain).reshape(-1, width)
    query = jnp.dot(flat, qkv_part[0], preferred_element_type=jnp.float32)
    key = jnp.dot(flat, qkv_part[1], preferred_element_type=jnp.float32)
    value = jnp.dot(flat, qkv_part[2], preferred_element_type=jnp.float32)
    mixed = attend(query, key, value, shape)
    update = jnp.dot(mixed, out_part, preferred_element_type=jnp.float32).reshape(tokens.shape)
    return (tokens.astype(jnp.float32) + update).astype(jnp.bfloat16)

def reference(video, norm_gain, qkv_weight, out_weight):
    frames, rows, cols, width = video.shape
    state = sublayer(video.reshape(1, frames, rows * cols, width), norm_gain[0], qkv_weight[0], out_weight[0]).reshape(video.shape)

    def across(frame):
        return sublayer(frame.reshape(rows, cols, 1, width), norm_gain[1], qkv_weight[1], out_weight[1]).reshape(frame.shape)
    state = lax.map(across, state)

    def downward(frame):
        return sublayer(frame.reshape(1, rows, cols, width), norm_gain[2], qkv_weight[2], out_weight[2]).reshape(frame.shape)
    return lax.map(downward, state)
```

```python
import functools
import math

import jax
import jax.numpy as jnp
from jax import lax
from jax.experimental import pallas as pl
from jax.experimental.pallas import tpu as pltpu
from jax.sharding import PartitionSpec as P

HEAD_DIM = 64
EPSILON = 1e-06
PAIR = 2 * HEAD_DIM
MESH = pl.DeviceIdType.MESH
F32, BF16 = jnp.float32, jnp.bfloat16
CROSS = (((1,), (1,)), ((), ()))


def iota(shape, dim):
    return lax.broadcasted_iota(jnp.int32, shape, dim)


def one_hot(condition):
    return jnp.where(condition, 1.0, 0.0).astype(BF16)


def matmul(a, b):
    return jnp.dot(a, b, preferred_element_type=F32)


def kernel(side, video_hbm, gain_ref, wqkv_hbm, wo_hbm, out_ref,
           x0, x1, x2, normed, qkv, mixed, wqkv, wo,
           sa1, sb1, ra1, rb1, sa2, sb2, ra2, rb2,
           ta1, tb1, ua1, ub1, ta2, tb2, ub2,
           local_sem, wsend, wrecv, ssem, rsem):
    frames, rows, width = x0.shape
    half = width // 2
    pairs = half // PAIR
    chunks = ra1.shape[0]
    band = rows // chunks
    count = frames * band
    tok, s = lax.axis_index("tok"), lax.axis_index("sub")
    o = 1 - s
    gx, gy = tok // side, lax.rem(tok, side)
    slot_x, slot_y = gx * 2 + s, gy * 2 + s

    def other(g, k):
        return lax.rem(g + k, side)

    def at_x(g, core):
        return {"tok": g * side + gy, "sub": core}

    def at_y(g, core):
        return {"tok": gx * side + g, "sub": core}

    i, j = iota((count, count), 0), iota((count, count), 1)
    two = 2 * side
    swap_lines = one_hot(j == lax.rem(i // 2, side) * two + (i // two) * 2 + lax.rem(i, 2))
    group = one_hot(j == lax.rem(i, side) * two + i // side)
    ungroup = one_hot(j == lax.rem(i, two) * side + i // two)
    swap_tokens = one_hot(j == lax.rem(i, side) * two + lax.rem(i // side, 2) * side + i // two)

    load_x = pltpu.make_async_copy(video_hbm, x0, local_sem.at[0])
    load_x.start()

    def load_w(l):
        return (pltpu.make_async_copy(wqkv_hbm.at[l], wqkv.at[l, s], local_sem.at[1 + 2 * l]),
                pltpu.make_async_copy(wo_hbm.at[l], wo.at[l, s], local_sem.at[2 + 2 * l]))

    def pass_w(l, part):
        if part < 3:
            return pltpu.make_async_remote_copy(
                wqkv_hbm.at[l, part], wqkv.at[l, s, part], wsend.at[l, part], wrecv.at[l, part],
                device_id={"sub": o}, device_id_type=MESH)
        return pltpu.make_async_remote_copy(
            wo_hbm.at[l], wo.at[l, s], wsend.at[l, 3], wrecv.at[l, 3],
            device_id={"sub": o}, device_id_type=MESH)

    for l in range(3):
        for copy in load_w(l):
            copy.start()
    barrier = pltpu.get_barrier_semaphore()
    pl.semaphore_signal(barrier, inc=1, device_id={"sub": o}, device_id_type=MESH)
    for k in range(1, side):
        for core in range(2):
            pl.semaphore_signal(barrier, inc=1, device_id=at_x(other(gx, k), core), device_id_type=MESH)
            pl.semaphore_signal(barrier, inc=1, device_id=at_y(other(gy, k), core), device_id_type=MESH)

    lane = iota((1, PAIR), 1)
    left, right = one_hot(lane < HEAD_DIM), one_hot(lane >= HEAD_DIM)
    r, c2 = iota((PAIR, PAIR), 0), iota((PAIR, PAIR), 1)
    mean_heads = (jnp.where(r // HEAD_DIM == c2 // HEAD_DIM, 1.0 / HEAD_DIM, 0.0)).astype(BF16)

    def span(c):
        return pl.ds(pl.multiple_of(c * band, band), band)

    def normalize(src, l, c):
        values = src[:, span(c), :].reshape(count, width).astype(F32)
        scale = lax.rsqrt(jnp.mean(values * values, axis=-1, keepdims=True) + EPSILON)
        out = (values * scale * gain_ref[l:l + 1, :]).astype(BF16)
        normed[:, span(c), :] = out.reshape(frames, band, width)

    def project(l, c, h):
        flat = normed[:, span(c), :].reshape(count, width)
        for part in range(3):
            y = matmul(flat, wqkv[l, h, part])
            if part < 2:
                square = (y * y).astype(BF16)
                y = jnp.concatenate([
                    y[:, p * PAIR:(p + 1) * PAIR] * lax.rsqrt(
                        matmul(square[:, p * PAIR:(p + 1) * PAIR], mean_heads) + EPSILON)
                    for p in range(pairs)], axis=1)
            qkv[part, h, :, span(c), :] = y.astype(BF16).reshape(frames, band, half)

    def attend_pair(q, k, v, mask):
        n = q.shape[0]
        kk = jnp.concatenate([k * left, k * right], axis=0)
        scores = lax.dot_general(q, kk, CROSS, preferred_element_type=F32)
        expo = jnp.exp2(scores * (math.log2(math.e) / math.sqrt(HEAD_DIM)))
        if mask is not None:
            expo = expo * mask
        ones = jnp.concatenate([jnp.broadcast_to(left, (n, PAIR)), jnp.broadcast_to(right, (n, PAIR))], axis=0)
        vv = jnp.concatenate([jnp.concatenate([v * left, v * right], axis=0), ones], axis=1)
        both = matmul(expo.astype(BF16), vv)
        return (both[:, :PAIR] / both[:, PAIR:]).astype(BF16)

    def attend(c, h, mask):
        for p in range(pairs):
            lanes = slice(p * PAIR, (p + 1) * PAIR)
            q, k, v = (qkv[part, h, :, span(c), lanes].reshape(count, PAIR) for part in range(3))
            mixed[h, :, span(c), lanes] = attend_pair(q, k, v, mask).reshape(frames, band, PAIR)

    def output(src, l, c):
        total = src[:, span(c), :].reshape(count, width).astype(F32)
        update = (matmul(mixed[0, :, span(c), :].reshape(count, half), wo[l, 0])
                  + matmul(mixed[1, :, span(c), :].reshape(count, half), wo[l, 1]))
        return (total + update).astype(BF16)

    def permute(matrix, values):
        return matmul(matrix, values).astype(BF16)

    order = sorted(range(1, side), key=lambda k: -min(k, side - k))

    def ring(send, recv, sem, c, me, place):
        for k in order:
            g = other(me, k)
            pltpu.make_async_remote_copy(
                send.at[c, g], recv.at[c, me], ssem.at[sem, c], rsem.at[sem, c],
                device_id=place(g, s), device_id_type=MESH).start()
        recv[c, me] = send[c, me]

    def fan(send, recv, sem, c, me, slot, place):
        for k in order:
            g = other(me, k)
            for core in range(2):
                pltpu.make_async_remote_copy(
                    send.at[c, g * 2 + core], recv.at[c, slot], ssem.at[sem, c], rsem.at[sem, c],
                    device_id=place(g, core), device_id_type=MESH).start()
        pltpu.make_async_remote_copy(
            send.at[c, me * 2 + o], recv.at[c, slot], ssem.at[sem, c], rsem.at[sem, c],
            device_id={"sub": o}, device_id_type=MESH).start()
        recv[c, slot] = send[c, slot]

    def arrived(recv, sem, c):
        pieces = recv.at[c, pl.ds(0, recv.shape[1] - 1)]
        pltpu.make_async_copy(pieces, pieces, rsem.at[sem, c]).wait()

    def sent(send, sem, c):
        pieces = send.at[c, pl.ds(0, send.shape[1] - 1)]
        pltpu.make_async_copy(pieces, pieces, ssem.at[sem, c]).wait()

    def flat(recv, c):
        return recv[c].reshape(count, half)

    def start_out(c, values):
        sa1[c] = values[:, :half].reshape(side, two, half)
        sb1[c] = permute(swap_lines, values[:, half:]).reshape(side, two, half)
        ring(sa1, ra1, 0, c, gx, at_x)
        ring(sb1, rb1, 1, c, gy, at_y)

    def relay_out(c):
        arrived(ra1, 0, c)
        sa2[c] = permute(group, flat(ra1, c)).reshape(two, side, half)
        fan(sa2, ra2, 2, c, gy, slot_y, at_y)
        arrived(rb1, 1, c)
        sb2[c] = permute(group, flat(rb1, c)).reshape(two, side, half)
        fan(sb2, rb2, 3, c, gx, slot_x, at_x)

    def finish_out(c):
        arrived(ra2, 2, c)
        x1[:, span(c), 0:half] = flat(ra2, c).reshape(frames, band, half)
        arrived(rb2, 3, c)
        x1[:, span(c), half:width] = permute(swap_tokens, flat(rb2, c)).reshape(frames, band, half)

    def start_back(c, values):
        ta1[c] = values[:, :half].reshape(two, side, half)
        tb1[c] = permute(swap_tokens, values[:, half:]).reshape(two, side, half)
        fan(ta1, ua1, 4, c, gy, slot_y, at_y)
        fan(tb1, ub1, 5, c, gx, slot_x, at_x)

    def relay_back(c):
        arrived(ua1, 4, c)
        ta2[c] = permute(ungroup, flat(ua1, c)).reshape(side, two, half)
        for k in order:
            g = other(gx, k)
            pltpu.make_async_remote_copy(
                ta2.at[c, g], x2.at[gx, span(c), pl.ds(0, half)], ssem.at[6, c], rsem.at[6, c],
                device_id=at_x(g, s), device_id_type=MESH).start()
        x2[gx, span(c), 0:half] = ta2[c, gx]
        arrived(ub1, 5, c)
        tb2[c] = permute(ungroup, flat(ub1, c)).reshape(side, two, half)
        ring(tb2, ub2, 7, c, gy, at_y)

    def finish_back(c):
        sent_like = ta2.at[c, pl.ds(0, side - 1)]
        pltpu.make_async_copy(sent_like, sent_like, rsem.at[6, c]).wait()
        arrived(ub2, 7, c)
        x2[:, span(c), half:width] = permute(swap_lines, flat(ub2, c)).reshape(frames, band, half)

    load_x.wait()
    for copy in load_w(0):
        copy.wait()

    @pl.loop(0, chunks)
    def _(c):
        normalize(x0, 0, c)
        project(0, c, s)

    pl.semaphore_wait(barrier, 4 * (side - 1) + 1)
    for l in range(2):
        for part in range(4):
            pass_w(l, part).start()
    i2, j2 = iota((count, 2 * count), 0), iota((count, 2 * count), 1)
    same_row = jnp.where(lax.rem(i2, band) == lax.rem(j2, band), 1.0, 0.0)

    @pl.loop(0, chunks)
    def _(c):
        attend(c, s, same_row)

    for part in range(3):
        pass_w(0, part).wait_recv()

    @pl.loop(0, chunks)
    def _(c):
        project(0, c, o)
        attend(c, o, same_row)

        @pl.when(c == 0)
        def _():
            pass_w(0, 3).wait_recv()

        start_out(c, output(x0, 0, c))

        @pl.when(c > 0)
        def _():
            relay_out(c - 1)

    relay_out(chunks - 1)
    for part in range(4):
        pass_w(2, part).start()

    for copy in load_w(1):
        copy.wait()
    for part in range(4):
        pass_w(1, part).wait_recv()

    @pl.loop(0, chunks)
    def _(c):
        finish_out(c)
        normalize(x1, 1, c)
        for h in range(2):
            project(1, c, h)
            attend(c, h, None)
        start_back(c, output(x1, 1, c))

        @pl.when(c > 0)
        def _():
            relay_back(c - 1)

    relay_back(chunks - 1)

    for copy in load_w(2):
        copy.wait()
    for part in range(4):
        pass_w(2, part).wait_recv()

    @pl.loop(0, chunks)
    def _(c):
        finish_back(c)
        normalize(x2, 2, c)
        for h in range(2):
            project(2, c, h)

    @pl.loop(0, frames)
    def _(f):
        for h in range(2):
            for p in range(pairs):
                lanes = slice(p * PAIR, (p + 1) * PAIR)
                mixed[h, f, :, lanes] = attend_pair(qkv[0, h, f, :, lanes], qkv[1, h, f, :, lanes], qkv[2, h, f, :, lanes], None)

    @pl.loop(0, chunks)
    def _(c):
        out_ref[:, span(c), :] = output(x2, 2, c).reshape(frames, band, width)

    for l in range(3):
        for part in range(4):
            pass_w(l, part).wait_send()

    @pl.loop(0, chunks)
    def _(c):
        for sem, send in enumerate((sa1, sb1, sa2, sb2, ta1, tb1, ta2, tb2)):
            sent(send, sem, c)


def body(side, video, norm_gain, qkv_weight, out_weight):
    frames, rows, cols, width = video.shape
    half = width // 2
    lines = 2 * side * side
    chunks = frames * rows // lines
    ring = pltpu.VMEM((chunks, side, 2 * side, half), BF16)
    fan = pltpu.VMEM((chunks, 2 * side, side, half), BF16)
    tokens = pltpu.VMEM((frames, rows, width), BF16)
    dma = pltpu.SemaphoreType.DMA
    anywhere = pl.BlockSpec(memory_space=pl.ANY)
    vmem = pl.BlockSpec(memory_space=pltpu.VMEM)
    out = pl.pallas_call(
        functools.partial(kernel, side),
        out_shape=jax.ShapeDtypeStruct((frames, rows, width), BF16),
        in_specs=[anywhere, vmem, anywhere, anywhere],
        out_specs=vmem,
        scratch_shapes=[
            tokens, tokens, tokens, tokens,
            pltpu.VMEM((3, 2, frames, rows, half), BF16),
            pltpu.VMEM((2, frames, rows, half), BF16),
            pltpu.VMEM((3, 2, 3, width, half), BF16),
            pltpu.VMEM((3, 2, half, width), BF16),
            ring, ring, ring, ring, fan, fan, fan, fan,
            fan, fan, fan, fan, ring, ring, ring,
            dma((7,)), dma((3, 4)), dma((3, 4)), dma((8, chunks)), dma((8, chunks)),
        ],
        compiler_params=pltpu.CompilerParams(
            collective_id=0, has_side_effects=True, vmem_limit_bytes=60 * 1024 * 1024),
    )(video.reshape(frames, rows, width), norm_gain, qkv_weight, out_weight)
    return out.reshape(video.shape)


def solution(mesh):
    side = math.isqrt(mesh.shape["tok"])
    in_specs = (
        P("parts", None, ("tok", "sub"), None),
        P(),
        P(None, None, None, "sub"),
        P(None, "sub", None),
    )
    out_specs = P("parts", None, ("tok", "sub"), None)
    return jax.shard_map(functools.partial(body, side), mesh=mesh, in_specs=in_specs, out_specs=out_specs, check_vma=False)
```

```python
import functools
import math

import jax
import jax.numpy as jnp
from jax import lax
from jax.experimental import pallas as pl
from jax.experimental.pallas import tpu as pltpu
from jax.sharding import PartitionSpec as P

HEAD_DIM = 64
EPSILON = 1e-06
PAIR = 2 * HEAD_DIM
MESH = pl.DeviceIdType.MESH
F32, BF16 = jnp.float32, jnp.bfloat16
CROSS = (((1,), (1,)), ((), ()))


def iota(shape, dim):
    return lax.broadcasted_iota(jnp.int32, shape, dim)


def one_hot(condition):
    return jnp.where(condition, 1.0, 0.0).astype(BF16)


def matmul(a, b):
    return jnp.dot(a, b, preferred_element_type=F32)


def kernel(side, video_hbm, gain_ref, wqkv_hbm, wo_hbm, out_ref,
           x0, x1, x2, normed, qkv, mixed, own, give, take,
           w0, wo0, wide, wide_o, mean_heads, ones, row_mask,
           sa1, sb1, ra1, rb1, sa2, sb2, ra2, rb2,
           ta1, tb1, ua1, ub1, ta2, tb2, ub2,
           local_sem, pair_sem, wsend, wrecv, ssem, rsem):
    frames, rows, width = x0.shape
    half = width // 2
    pairs = width // PAIR
    chunks = ra1.shape[0]
    band = rows // chunks
    count = frames * band
    tile = 2 * PAIR
    tok, s = lax.axis_index("tok"), lax.axis_index("sub")
    o = 1 - s
    gx, gy = tok // side, lax.rem(tok, side)
    slot_x, slot_y = gx * 2 + s, gy * 2 + s
    partner = {"sub": o}

    def other(g, k):
        return lax.rem(g + k, side)

    def at_x(g, core):
        return {"tok": g * side + gy, "sub": core}

    def at_y(g, core):
        return {"tok": gx * side + g, "sub": core}

    load_x = pltpu.make_async_copy(video_hbm, x0, local_sem.at[0])
    load_x.start()
    load_0 = [pltpu.make_async_copy(wqkv_hbm.at[0, part], w0.at[:, pl.ds(part * half, half)], local_sem.at[1 + part])
              for part in range(3)]
    load_0.append(pltpu.make_async_copy(wo_hbm.at[0], wo0, local_sem.at[4]))
    for copy in load_0:
        copy.start()
    mine = pl.multiple_of(s * half, half)

    def own_w(l):
        base = 5 + 4 * (l - 1)
        copies = [pltpu.make_async_copy(
            wqkv_hbm.at[l, part], wide.at[l - 1, :, pl.ds(part * width + mine, half)], local_sem.at[base + part])
            for part in range(3)]
        copies.append(pltpu.make_async_copy(wo_hbm.at[l], wide_o.at[l - 1, pl.ds(mine, half), :], local_sem.at[base + 3]))
        return copies

    def pass_w(l):
        copies = [pltpu.make_async_remote_copy(
            wqkv_hbm.at[l, part], wide.at[l - 1, :, pl.ds(part * width + mine, half)],
            wsend.at[l - 1, part], wrecv.at[l - 1, part], device_id=partner, device_id_type=MESH)
            for part in range(3)]
        copies.append(pltpu.make_async_remote_copy(
            wo_hbm.at[l], wide_o.at[l - 1, pl.ds(mine, half), :],
            wsend.at[l - 1, 3], wrecv.at[l - 1, 3], device_id=partner, device_id_type=MESH))
        return copies

    barrier = pltpu.get_barrier_semaphore()
    pl.semaphore_signal(barrier, inc=1, device_id=partner, device_id_type=MESH)
    for k in range(1, side):
        for core in range(2):
            pl.semaphore_signal(barrier, inc=1, device_id=at_x(other(gx, k), core), device_id_type=MESH)
            pl.semaphore_signal(barrier, inc=1, device_id=at_y(other(gy, k), core), device_id_type=MESH)
    for l in (1, 2):
        for copy in own_w(l):
            copy.start()

    i, j = iota((count, count), 0), iota((count, count), 1)
    two = 2 * side
    swap_lines = one_hot(j == lax.rem(i // 2, side) * two + (i // two) * 2 + lax.rem(i, 2))
    group = one_hot(j == lax.rem(i, side) * two + i // side)
    ungroup = one_hot(j == lax.rem(i, two) * side + i // two)
    swap_tokens = one_hot(j == lax.rem(i, side) * two + lax.rem(i // side, 2) * side + i // two)

    lane = iota((1, PAIR), 1)
    left, right = one_hot(lane < HEAD_DIM), one_hot(lane >= HEAD_DIM)
    r, c2 = iota((tile, tile), 0), iota((tile, tile), 1)
    mean_heads[...] = jnp.where(r // HEAD_DIM == c2 // HEAD_DIM, 1.0 / HEAD_DIM, 0.0).astype(BF16)
    i2, j2 = iota((count, 2 * count), 0), iota((count, 2 * count), 1)
    row_mask[...] = one_hot(lax.rem(i2, band) == lax.rem(j2, band))
    r, c2 = iota((2 * count, PAIR), 0), iota((2 * count, PAIR), 1)
    ones[...] = one_hot(r // count == c2 // HEAD_DIM)

    def span(c):
        return pl.ds(pl.multiple_of(c * band, band), band)

    def normalize(tokens, l):
        values = tokens.astype(F32)
        scale = lax.rsqrt(jnp.mean(values * values, axis=-1, keepdims=True) + EPSILON)
        return (values * scale * gain_ref[l:l + 1, :]).astype(BF16)

    def project(flat, w, total, scaled):
        every, tiles = matmul(flat, w[...]), []
        for start in range(0, total, tile):
            y = every[:, start:min(start + tile, total)]
            if start < scaled:
                y = y * lax.rsqrt(matmul((y * y).astype(BF16), mean_heads[...]) + EPSILON)
            tiles.append(y.astype(BF16))
        return tiles

    def pair_of(tiles, p):
        return tiles[p // 2][:, (p % 2) * PAIR:(p % 2 + 1) * PAIR]

    def attend(queries, keys, values, sums, mask):
        scores = [lax.dot_general(q, jnp.concatenate([k * left, k * right], axis=0), CROSS, preferred_element_type=F32)
                  for q, k in zip(queries, keys)]
        expos = [jnp.exp2(score * (math.log2(math.e) / math.sqrt(HEAD_DIM))).astype(BF16) for score in scores]
        if mask is not None:
            expos = [expo * mask for expo in expos]
        outs = []
        for expo, v in zip(expos, values):
            vv = jnp.concatenate([jnp.concatenate([v * left, v * right], axis=0), sums], axis=1)
            both = matmul(expo, vv)
            outs.append((both[:, :PAIR] / both[:, PAIR:]).astype(BF16))
        return jnp.concatenate(outs, axis=1)

    def attention(tiles, n, mask):
        split = [pair_of(tiles, p) for p in range(3 * n)]
        return attend(split[:n], split[n:2 * n], split[2 * n:], ones[...], mask)

    def permute(matrix, values):
        return matmul(matrix, values).astype(BF16)

    order = sorted(range(1, side), key=lambda k: -min(k, side - k))

    def ring(send, recv, sem, c, me, place):
        for k in order:
            g = other(me, k)
            pltpu.make_async_remote_copy(
                send.at[c, g], recv.at[c, me], ssem.at[sem, c], rsem.at[sem, c],
                device_id=place(g, s), device_id_type=MESH).start()
        recv[c, me] = send[c, me]

    def fan(send, recv, sem, c, me, slot, place):
        for k in order:
            g = other(me, k)
            for core in range(2):
                pltpu.make_async_remote_copy(
                    send.at[c, g * 2 + core], recv.at[c, slot], ssem.at[sem, c], rsem.at[sem, c],
                    device_id=place(g, core), device_id_type=MESH).start()
        pltpu.make_async_remote_copy(
            send.at[c, me * 2 + o], recv.at[c, slot], ssem.at[sem, c], rsem.at[sem, c],
            device_id=partner, device_id_type=MESH).start()
        recv[c, slot] = send[c, slot]

    def arrived(recv, sem, c):
        pieces = recv.at[c, pl.ds(0, recv.shape[1] - 1)]
        pltpu.make_async_copy(pieces, pieces, rsem.at[sem, c]).wait()

    def sent(send, sem, c):
        pieces = send.at[c, pl.ds(0, send.shape[1] - 1)]
        pltpu.make_async_copy(pieces, pieces, ssem.at[sem, c]).wait()

    def flat(recv, c):
        return recv[c].reshape(count, half)

    def start_out(c, values):
        sa1[c] = values[:, :half].reshape(side, two, half)
        sb1[c] = permute(swap_lines, values[:, half:]).reshape(side, two, half)
        ring(sa1, ra1, 0, c, gx, at_x)
        ring(sb1, rb1, 1, c, gy, at_y)

    def relay_out(c):
        arrived(ra1, 0, c)
        arrived(rb1, 1, c)
        sa2[c] = permute(group, flat(ra1, c)).reshape(two, side, half)
        sb2[c] = permute(group, flat(rb1, c)).reshape(two, side, half)
        fan(sa2, ra2, 2, c, gy, slot_y, at_y)
        fan(sb2, rb2, 3, c, gx, slot_x, at_x)

    def finish_out(c):
        arrived(ra2, 2, c)
        arrived(rb2, 3, c)
        return jnp.concatenate([flat(ra2, c), permute(swap_tokens, flat(rb2, c))], axis=1)

    def start_back(c, values):
        ta1[c] = values[:, :half].reshape(two, side, half)
        tb1[c] = permute(swap_tokens, values[:, half:]).reshape(two, side, half)
        fan(ta1, ua1, 4, c, gy, slot_y, at_y)
        fan(tb1, ub1, 5, c, gx, slot_x, at_x)

    def relay_back(c):
        arrived(ua1, 4, c)
        arrived(ub1, 5, c)
        tb2[c] = permute(ungroup, flat(ub1, c)).reshape(side, two, half)
        ta2[c] = permute(ungroup, flat(ua1, c)).reshape(side, two, half)
        for k in order:
            g = other(gx, k)
            pltpu.make_async_remote_copy(
                ta2.at[c, g], x2.at[gx, span(c), pl.ds(0, half)], ssem.at[6, c], rsem.at[6, c],
                device_id=at_x(g, s), device_id_type=MESH).start()
        x2[gx, span(c), 0:half] = ta2[c, gx]
        ring(tb2, ub2, 7, c, gy, at_y)

    def finish_back(c):
        sent_like = ta2.at[c, pl.ds(0, side - 1)]
        pltpu.make_async_copy(sent_like, sent_like, rsem.at[6, c]).wait()
        arrived(ub2, 7, c)
        x2[:, span(c), half:width] = permute(swap_lines, flat(ub2, c)).reshape(frames, band, half)

    def pass_normed(c):
        return pltpu.make_async_remote_copy(
            normed.at[0, :, span(c), :], normed.at[1, :, span(c), :], pair_sem.at[0, c], pair_sem.at[1, c],
            device_id=partner, device_id_type=MESH)

    def pass_update(c):
        return pltpu.make_async_remote_copy(
            give.at[c], take.at[c], pair_sem.at[2, c], pair_sem.at[3, c], device_id=partner, device_id_type=MESH)

    def heads(slot, c):
        tiles = project(normed[slot, :, span(c), :].reshape(count, width), w0, 3 * half, width)
        return matmul(attention(tiles, pairs // 2, row_mask[...]), wo0[...])

    load_x.wait()

    @pl.loop(0, chunks)
    def _(c):
        normed[0, :, span(c), :] = normalize(x0[:, span(c), :].reshape(count, width), 0).reshape(frames, band, width)

    for copy in load_0:
        copy.wait()

    @pl.loop(0, chunks)
    def _(c):
        own[c] = x0[:, span(c), :].reshape(count, width).astype(F32) + heads(0, c)

    pl.semaphore_wait(barrier, 4 * (side - 1) + 1)
    for c in range(chunks):
        pass_normed(c).start()

    @pl.loop(0, chunks)
    def _(c):
        pass_normed(c).wait_recv()
        give[c] = heads(1, c).astype(BF16)
        pass_update(c).start()

    @pl.loop(0, chunks)
    def _(c):
        pass_update(c).wait_recv()
        start_out(c, (own[c] + take[c].astype(F32)).astype(BF16))

    for copy in pass_w(1):
        copy.start()

    @pl.loop(0, chunks)
    def _(c):
        relay_out(c)

    for copy in pass_w(2):
        copy.start()

    for copy in own_w(1):
        copy.wait()
    for copy in pass_w(1):
        copy.wait_recv()

    @pl.loop(0, chunks)
    def _(c):
        line = finish_out(c)
        tiles = project(normalize(line, 1), wide.at[0], 3 * width, 2 * width)
        update = matmul(attention(tiles, pairs, None), wide_o[0])
        start_back(c, (line.astype(F32) + update).astype(BF16))

        @pl.when(c > 0)
        def _():
            relay_back(c - 1)

    def columns(c):
        finish_back(c)
        tiles = project(normalize(x2[:, span(c), :].reshape(count, width), 2), wide.at[1], 3 * width, 2 * width)
        for t, value in enumerate(tiles):
            part, at = divmod(t * tile, width)
            qkv[part, :, span(c), at:at + tile] = value.reshape(frames, band, tile)

    for copy in own_w(2):
        copy.wait()
    for copy in pass_w(2):
        copy.wait_recv()

    @pl.loop(0, chunks)
    def _(c):
        columns(c)

        @pl.when(c == 0)
        def _():
            relay_back(chunks - 1)

    sums = jnp.concatenate([jnp.broadcast_to(left, (rows, PAIR)), jnp.broadcast_to(right, (rows, PAIR))], axis=0)

    lanes = [slice(p * PAIR, (p + 1) * PAIR) for p in range(pairs)]

    @pl.loop(0, frames // 2)
    def _(f2):
        for f in (2 * f2, 2 * f2 + 1):
            mixed[f] = attend(*([qkv[part, f, :, at] for at in lanes] for part in range(3)), sums, None)

    @pl.loop(0, chunks)
    def _(c):
        total = x2[:, span(c), :].reshape(count, width).astype(F32) + matmul(
            mixed[:, span(c), :].reshape(count, width), wide_o[1])
        out_ref[:, span(c), :] = total.astype(BF16).reshape(frames, band, width)

    for l in (1, 2):
        for copy in pass_w(l):
            copy.wait_send()

    @pl.loop(0, chunks)
    def _(c):
        pass_normed(c).wait_send()
        pass_update(c).wait_send()
        for sem, send in enumerate((sa1, sb1, sa2, sb2, ta1, tb1, ta2, tb2)):
            sent(send, sem, c)


def body(side, video, norm_gain, qkv_weight, out_weight):
    frames, rows, cols, width = video.shape
    half = width // 2
    lines = 2 * side * side
    chunks = frames * rows // lines
    count = frames * rows // chunks
    ring = pltpu.VMEM((chunks, side, 2 * side, half), BF16)
    fan = pltpu.VMEM((chunks, 2 * side, side, half), BF16)
    tokens = pltpu.VMEM((frames, rows, width), BF16)
    dma = pltpu.SemaphoreType.DMA
    anywhere = pl.BlockSpec(memory_space=pltpu.HBM)
    vmem = pl.BlockSpec(memory_space=pltpu.VMEM)
    out = pl.pallas_call(
        functools.partial(kernel, side),
        out_shape=jax.ShapeDtypeStruct((frames, rows, width), BF16),
        in_specs=[anywhere, vmem, anywhere, anywhere],
        out_specs=vmem,
        scratch_shapes=[
            tokens, tokens, tokens,
            pltpu.VMEM((2, frames, rows, width), BF16),
            pltpu.VMEM((3, frames, rows, width), BF16),
            tokens,
            pltpu.VMEM((chunks, count, width), F32),
            pltpu.VMEM((chunks, count, width), BF16), pltpu.VMEM((chunks, count, width), BF16),
            pltpu.VMEM((width, 3 * half), BF16), pltpu.VMEM((half, width), BF16),
            pltpu.VMEM((2, width, 3 * width), BF16), pltpu.VMEM((2, width, width), BF16),
            pltpu.VMEM((2 * PAIR, 2 * PAIR), BF16), pltpu.VMEM((2 * count, PAIR), BF16),
            pltpu.VMEM((count, 2 * count), BF16),
            ring, ring, ring, ring, fan, fan, fan, fan,
            fan, fan, fan, fan, ring, ring, ring,
            dma((13,)), dma((4, chunks)), dma((2, 4)), dma((2, 4)), dma((8, chunks)), dma((8, chunks)),
        ],
        compiler_params=pltpu.CompilerParams(
            collective_id=0, has_side_effects=True, vmem_limit_bytes=50 * 1024 * 1024),
    )(*(pltpu.with_memory_space_constraint(a, pltpu.HBM) for a in (video.reshape(frames, rows, width), norm_gain, qkv_weight, out_weight)))
    return out.reshape(video.shape)


def solution(mesh):
    side = math.isqrt(mesh.shape["tok"])
    in_specs = (
        P("parts", None, ("tok", "sub"), None),
        P(),
        P(None, None, None, "sub"),
        P(None, "sub", None),
    )
    out_specs = P("parts", None, ("tok", "sub"), None)
    return jax.shard_map(functools.partial(body, side), mesh=mesh, in_specs=in_specs, out_specs=out_specs, check_vma=False)
```

```python
import functools
import math

import jax
import jax.numpy as jnp
from jax import lax
from jax.experimental import pallas as pl
from jax.experimental.pallas import tpu as pltpu
from jax.sharding import PartitionSpec as P

HEAD_DIM = 64
EPSILON = 1e-06
PAIR = 2 * HEAD_DIM
MESH = pl.DeviceIdType.MESH
F32, BF16 = jnp.float32, jnp.bfloat16
CROSS = (((1,), (1,)), ((), ()))


def iota(shape, dim):
    return lax.broadcasted_iota(jnp.int32, shape, dim)


def one_hot(condition):
    return jnp.where(condition, 1.0, 0.0).astype(BF16)


def matmul(a, b):
    return jnp.dot(a, b, preferred_element_type=F32)


def kernel(side, video_hbm, gain_ref, wqkv_hbm, wo_hbm, out_ref,
           x0, x2, normed, qkv, mixed, own, give, take,
           w0, wo0, wide, wide_o, mean_heads, ones, row_mask,
           out1, in1, out2, in2, back1, land1, back2,
           local_sem, pair_sem, wsend, wrecv, ssem, rsem):
    frames, rows, width = x0.shape
    half = width // 2
    pairs = width // PAIR
    chunks = in1.shape[0]
    band = rows // chunks
    count = frames * band
    tile = 2 * PAIR
    tok, s = lax.axis_index("tok"), lax.axis_index("sub")
    o = 1 - s
    gx, gy = tok // side, lax.rem(tok, side)
    last = gx * s + gy * o
    last_o = gx * o + gy * s
    partner = {"sub": o}

    def other(g, k):
        return lax.rem(g + k, side)

    def at_x(g, core):
        return {"tok": g * side + gy, "sub": core}

    def at_y(g, core):
        return {"tok": gx * side + g, "sub": core}

    order = sorted(range(1, side), key=lambda k: -min(k, side - k))
    load_x = pltpu.make_async_copy(video_hbm, x0, local_sem.at[0])
    load_x.start()
    barrier = pltpu.get_barrier_semaphore()
    pl.semaphore_signal(barrier, inc=1, device_id=partner, device_id_type=MESH)
    for k in order:
        for core in range(2):
            pl.semaphore_signal(barrier, inc=1, device_id=at_x(other(gx, k), core), device_id_type=MESH)
            pl.semaphore_signal(barrier, inc=1, device_id=at_y(other(gy, k), core), device_id_type=MESH)
    load_0 = [pltpu.make_async_copy(wqkv_hbm.at[0, part], w0.at[:, pl.ds(part * half, half)], local_sem.at[1 + part])
              for part in range(3)]
    load_0.append(pltpu.make_async_copy(wo_hbm.at[0], wo0, local_sem.at[4]))
    for copy in load_0:
        copy.start()
    mine = pl.multiple_of(s * half, half)

    def own_w(l):
        base = 5 + 4 * (l - 1)
        copies = [pltpu.make_async_copy(
            wqkv_hbm.at[l, part], wide.at[l - 1, :, pl.ds(part * width + mine, half)], local_sem.at[base + part])
            for part in range(3)]
        copies.append(pltpu.make_async_copy(wo_hbm.at[l], wide_o.at[l - 1, pl.ds(mine, half), :], local_sem.at[base + 3]))
        return copies

    def pass_w(l):
        copies = [pltpu.make_async_remote_copy(
            wqkv_hbm.at[l, part], wide.at[l - 1, :, pl.ds(part * width + mine, half)],
            wsend.at[l - 1, part], wrecv.at[l - 1, part], device_id=partner, device_id_type=MESH)
            for part in range(3)]
        copies.append(pltpu.make_async_remote_copy(
            wo_hbm.at[l], wide_o.at[l - 1, pl.ds(mine, half), :],
            wsend.at[l - 1, 3], wrecv.at[l - 1, 3], device_id=partner, device_id_type=MESH))
        return copies

    for l in (1, 2):
        for copy in own_w(l):
            copy.start()

    i, j = iota((count, count), 0), iota((count, count), 1)
    square = side * side
    turn = one_hot(j == (i // square) * square + lax.rem(i, side) * side + lax.rem(i, square) // side)

    lane = iota((1, PAIR), 1)
    left, right = one_hot(lane < HEAD_DIM), one_hot(lane >= HEAD_DIM)
    r, c2 = iota((tile, tile), 0), iota((tile, tile), 1)
    mean_heads[...] = jnp.where(r // HEAD_DIM == c2 // HEAD_DIM, 1.0 / HEAD_DIM, 0.0).astype(BF16)
    i2, j2 = iota((count, 2 * count), 0), iota((count, 2 * count), 1)
    row_mask[...] = one_hot(lax.rem(i2, band) == lax.rem(j2, band))
    r, c2 = iota((2 * count, PAIR), 0), iota((2 * count, PAIR), 1)
    ones[...] = one_hot(r // count == c2 // HEAD_DIM)

    def span(c):
        return pl.ds(pl.multiple_of(c * band, band), band)

    def normalize(tokens, l):
        values = tokens.astype(F32)
        scale = lax.rsqrt(jnp.mean(values * values, axis=-1, keepdims=True) + EPSILON)
        return (values * scale * gain_ref[l:l + 1, :]).astype(BF16)

    def project(flat, w, total, scaled):
        every, tiles = matmul(flat, w[...]), []
        for start in range(0, total, tile):
            y = every[:, start:min(start + tile, total)]
            if start < scaled:
                y = y * lax.rsqrt(matmul((y * y).astype(BF16), mean_heads[...]) + EPSILON)
            tiles.append(y.astype(BF16))
        return tiles

    def pair_of(tiles, p):
        return tiles[p // 2][:, (p % 2) * PAIR:(p % 2 + 1) * PAIR]

    def attend(queries, keys, values, sums, mask):
        scores = [lax.dot_general(q, jnp.concatenate([k * left, k * right], axis=0), CROSS, preferred_element_type=F32)
                  for q, k in zip(queries, keys)]
        expos = [jnp.exp2(score * (math.log2(math.e) / math.sqrt(HEAD_DIM))).astype(BF16) for score in scores]
        if mask is not None:
            expos = [expo * mask for expo in expos]
        outs = []
        for expo, v in zip(expos, values):
            vv = jnp.concatenate([jnp.concatenate([v * left, v * right], axis=0), sums], axis=1)
            both = matmul(expo, vv)
            outs.append((both[:, :PAIR] / both[:, PAIR:]).astype(BF16))
        return jnp.concatenate(outs, axis=1)

    def attention(tiles, n, mask):
        split = [pair_of(tiles, p) for p in range(3 * n)]
        return attend(split[:n], split[n:2 * n], split[2 * n:], ones[...], mask)

    def permute(matrix, values):
        return matmul(matrix, values).astype(BF16)

    def push(src, dst, sem, c, device):
        pltpu.make_async_remote_copy(src, dst, ssem.at[sem, c], rsem.at[sem, c], device_id=device, device_id_type=MESH).start()

    def arrived(ref, sem, c):
        pltpu.make_async_copy(ref, ref, rsem.at[sem, c]).wait()

    def sent(ref, sem, c):
        pltpu.make_async_copy(ref, ref, ssem.at[sem, c]).wait()

    def all_but(ref, c, n):
        return ref.at[c, pl.ds(0, n)]

    def turned(ref, c):
        return permute(turn, ref[c].reshape(count, width)).reshape(2 * side, side, width)

    def start_out(c, values):
        out1[c] = values.reshape(2 * side, side, width)
        for k in order:
            x, y = other(gx, k), other(gy, k)
            push(out1.at[c, x * 2], in1.at[c, gx], 0, c, at_x(x, s))
            push(out1.at[c, y * 2 + 1], in1.at[c, side + gy], 0, c, at_y(y, s))
        in1[c, gx] = out1[c, gx * 2]
        in1[c, side + gy] = out1[c, gy * 2 + 1]

    def relay_out(c):
        arrived(all_but(in1, c, 2 * side - 2), 0, c)
        out2[c] = turned(in1, c)
        for k in order:
            x, y = other(gx, k), other(gy, k)
            push(out2.at[c, y], in2.at[c, gy * 2 + s], 1, c, at_y(y, 0))
            push(out2.at[c, side + x], in2.at[c, gx * 2 + s], 1, c, at_x(x, 1))
        push(out2.at[c, o * side + last_o], in2.at[c, last_o * 2 + s], 1, c, partner)
        in2[c, last * 2 + s] = out2[c, s * side + last]

    def start_back(c, values):
        back1[c] = values.reshape(2 * side, side, width)
        for k in order:
            g = other(last, k)
            chip = s * (g * side + gy) + o * (gx * side + g)
            for core in range(2):
                push(back1.at[c, g * 2 + core], land1.at[c, s * side + last], 2, c, {"tok": chip, "sub": core})
        push(back1.at[c, last * 2 + o], land1.at[c, s * side + last], 2, c, partner)
        land1[c, s * side + last] = back1[c, last * 2 + s]

    def relay_back(c):
        arrived(all_but(land1, c, 2 * side - 1), 2, c)
        back2[c] = turned(land1, c)
        for k in order:
            x, y = other(gx, k), other(gy, k)
            push(back2.at[c, x], x2.at[gx, c, 0], 3, c, at_x(x, s))
            push(back2.at[c, side + y], x2.at[gy, c, 1], 3, c, at_y(y, s))
        x2[gx, c, 0] = back2[c, gx]
        x2[gy, c, 1] = back2[c, side + gy]

    def finish_back(c):
        arrived(all_but(back2, c, 2 * side - 2), 3, c)

    def pass_normed(c):
        return pltpu.make_async_remote_copy(
            normed.at[0, :, span(c), :], normed.at[1, :, span(c), :], pair_sem.at[0, c], pair_sem.at[1, c],
            device_id=partner, device_id_type=MESH)

    def pass_update(c):
        return pltpu.make_async_remote_copy(
            give.at[:, span(c), :], take.at[:, span(c), :], pair_sem.at[2, c], pair_sem.at[3, c],
            device_id=partner, device_id_type=MESH)

    def project_heads(slot):
        tiles = project(normed[slot].reshape(frames * rows, width), w0, 3 * half, width)
        for part in range(3):
            for p in range(pairs // 2):
                qkv[part, :, :, p * PAIR:(p + 1) * PAIR] = pair_of(tiles, part * (pairs // 2) + p).reshape(frames, rows, PAIR)

    def attend_heads():
        for c in range(chunks):
            at = slice(c * band, (c + 1) * band)
            split = [[qkv[part, :, at, p * PAIR:(p + 1) * PAIR].reshape(count, PAIR) for p in range(pairs // 2)]
                     for part in range(3)]
            mixed[:, at, 0:half] = attend(*split, ones[...], row_mask[...]).reshape(frames, band, half)
        return matmul(mixed[:, :, 0:half].reshape(frames * rows, half), wo0[...])

    load_x.wait()

    @pl.loop(0, chunks)
    def _(c):
        normed[0, :, span(c), :] = normalize(x0[:, span(c), :].reshape(count, width), 0).reshape(frames, band, width)

    for copy in load_0:
        copy.wait()

    project_heads(0)
    pl.semaphore_wait(barrier, 4 * (side - 1) + 1)
    for c in range(chunks):
        pass_normed(c).start()
    own[...] = x0[...].astype(F32) + attend_heads().reshape(frames, rows, width)

    def join(c):
        pass_update(c).wait_recv()
        at = slice(c * band, (c + 1) * band)
        start_out(c, (own[:, at, :] + take[:, at, :].astype(F32)).astype(BF16).reshape(count, width))

    for c in range(chunks):
        pass_normed(c).wait_recv()
        tiles = project(normed[1, :, c * band:(c + 1) * band, :].reshape(count, width), w0, 3 * half, width)
        update = matmul(attention(tiles, pairs // 2, row_mask[...]), wo0[...])
        give[:, c * band:(c + 1) * band, :] = update.astype(BF16).reshape(frames, band, width)
        pass_update(c).start()
        if c > 0:
            join(c - 1)
    join(chunks - 1)

    for copy in pass_w(1):
        copy.start()

    @pl.loop(0, chunks)
    def _(c):
        relay_out(c)

    for copy in pass_w(2):
        copy.start()

    for copy in own_w(1):
        copy.wait()
    for copy in pass_w(1):
        copy.wait_recv()

    @pl.loop(0, chunks)
    def _(c):
        arrived(all_but(in2, c, 2 * side - 1), 1, c)
        line = in2[c].reshape(count, width)
        tiles = project(normalize(line, 1), wide.at[0], 3 * width, 2 * width)
        update = matmul(attention(tiles, pairs, None), wide_o[0])
        start_back(c, (line.astype(F32) + update).astype(BF16))

    @pl.loop(0, chunks)
    def _(c):
        relay_back(c)

    def columns(c):
        finish_back(c)
        tiles = project(normalize(x2[:, c].reshape(count, width), 2), wide.at[1], 3 * width, 2 * width)
        for t, value in enumerate(tiles):
            part, at = divmod(t * tile, width)
            qkv[part, :, span(c), at:at + tile] = value.reshape(frames, band, tile)

    for copy in own_w(2):
        copy.wait()
    for copy in pass_w(2):
        copy.wait_recv()

    @pl.loop(0, chunks)
    def _(c):
        columns(c)

    sums = jnp.concatenate([jnp.broadcast_to(left, (rows, PAIR)), jnp.broadcast_to(right, (rows, PAIR))], axis=0)

    lanes = [slice(p * PAIR, (p + 1) * PAIR) for p in range(pairs)]

    @pl.loop(0, frames // 2)
    def _(f2):
        for f in (2 * f2, 2 * f2 + 1):
            mixed[f] = attend(*([qkv[part, f, :, at] for at in lanes] for part in range(3)), sums, None)

    total = x2[...].reshape(frames * rows, width).astype(F32) + matmul(mixed[...].reshape(frames * rows, width), wide_o[1])
    out_ref[...] = total.astype(BF16).reshape(frames, rows, width)

    for l in (1, 2):
        for copy in pass_w(l):
            copy.wait_send()

    @pl.loop(0, chunks)
    def _(c):
        pass_normed(c).wait_send()
        pass_update(c).wait_send()
        for sem, (ref, n) in enumerate(((out1, 2), (out2, 1), (back1, 1), (back2, 2))):
            sent(all_but(ref, c, 2 * side - n), sem, c)


def body(side, video, norm_gain, qkv_weight, out_weight):
    frames, rows, cols, width = video.shape
    half = width // 2
    lines = 2 * side * side
    chunks = frames * rows // lines
    count = frames * rows // chunks
    blocks = pltpu.VMEM((chunks, 2 * side, side, width), BF16)
    tokens = pltpu.VMEM((frames, rows, width), BF16)
    dma = pltpu.SemaphoreType.DMA
    anywhere = pl.BlockSpec(memory_space=pltpu.HBM)
    vmem = pl.BlockSpec(memory_space=pltpu.VMEM)
    out = pl.pallas_call(
        functools.partial(kernel, side),
        out_shape=jax.ShapeDtypeStruct((frames, rows, width), BF16),
        in_specs=[anywhere, vmem, anywhere, anywhere],
        out_specs=vmem,
        scratch_shapes=[
            tokens,
            pltpu.VMEM((frames, chunks, 2, side, width), BF16),
            pltpu.VMEM((2, frames, rows, width), BF16),
            pltpu.VMEM((3, frames, rows, width), BF16),
            tokens,
            pltpu.VMEM((frames, rows, width), F32), tokens, tokens,
            pltpu.VMEM((width, 3 * half), BF16), pltpu.VMEM((half, width), BF16),
            pltpu.VMEM((2, width, 3 * width), BF16), pltpu.VMEM((2, width, width), BF16),
            pltpu.VMEM((2 * PAIR, 2 * PAIR), BF16), pltpu.VMEM((2 * count, PAIR), BF16),
            pltpu.VMEM((count, 2 * count), BF16),
            blocks, blocks, blocks, blocks, blocks, blocks, blocks,
            dma((13,)), dma((4, chunks)), dma((2, 4)), dma((2, 4)), dma((4, chunks)), dma((4, chunks)),
        ],
        compiler_params=pltpu.CompilerParams(
            collective_id=0, has_side_effects=True, vmem_limit_bytes=50 * 1024 * 1024),
    )(*(pltpu.with_memory_space_constraint(a, pltpu.HBM) for a in (video.reshape(frames, rows, width), norm_gain, qkv_weight, out_weight)))
    return out.reshape(video.shape)


def solution(mesh):
    side = math.isqrt(mesh.shape["tok"])
    in_specs = (
        P("parts", None, ("tok", "sub"), None),
        P(),
        P(None, None, None, "sub"),
        P(None, "sub", None),
    )
    out_specs = P("parts", None, ("tok", "sub"), None)
    return jax.shard_map(functools.partial(body, side), mesh=mesh, in_specs=in_specs, out_specs=out_specs, check_vma=False)
```

```python
import functools
import math

import jax
import jax.numpy as jnp
from jax import lax
from jax.experimental import pallas as pl
from jax.experimental.pallas import tpu as pltpu
from jax.sharding import PartitionSpec as P

HEAD_DIM = 64
EPSILON = 1e-06
PAIR = 2 * HEAD_DIM
MESH = pl.DeviceIdType.MESH
F32, BF16 = jnp.float32, jnp.bfloat16
CROSS = (((1,), (1,)), ((), ()))


def iota(shape, dim):
    return lax.broadcasted_iota(jnp.int32, shape, dim)


def one_hot(condition):
    return jnp.where(condition, 1.0, 0.0).astype(BF16)


def matmul(a, b):
    return jnp.dot(a, b, preferred_element_type=F32)


def kernel(side, video_hbm, gain_ref, wqkv_hbm, wo_hbm, out_ref,
           x0, x2, normed, qkv, mixed, own, give, take,
           w0, wo0, wide, wide_o, mean_heads, ones, row_mask,
           out1, in1, out2, in2, back1, land1, back2,
           local_sem, pair_sem, wsend, wrecv, ssem, rsem):
    frames, rows, width = x0.shape
    half = width // 2
    pairs = width // PAIR
    chunks = in1.shape[0]
    band = rows // chunks
    count = frames * band
    tile = 2 * PAIR
    tok, s = lax.axis_index("tok"), lax.axis_index("sub")
    o = 1 - s
    gx, gy = tok // side, lax.rem(tok, side)
    last = gx * s + gy * o
    last_o = gx * o + gy * s
    partner = {"sub": o}

    def other(g, k):
        return lax.rem(g + k, side)

    def at_x(g, core):
        return {"tok": g * side + gy, "sub": core}

    def at_y(g, core):
        return {"tok": gx * side + g, "sub": core}

    order = sorted(range(1, side), key=lambda k: -min(k, side - k))
    load_x = pltpu.make_async_copy(video_hbm, x0, local_sem.at[0])
    load_x.start()
    barrier = pltpu.get_barrier_semaphore()
    pl.semaphore_signal(barrier, inc=1, device_id=partner, device_id_type=MESH)
    for k in order:
        for core in range(2):
            pl.semaphore_signal(barrier, inc=1, device_id=at_x(other(gx, k), core), device_id_type=MESH)
            pl.semaphore_signal(barrier, inc=1, device_id=at_y(other(gy, k), core), device_id_type=MESH)
    load_0 = [pltpu.make_async_copy(wqkv_hbm.at[0, part], w0.at[:, pl.ds(part * half, half)], local_sem.at[1 + part])
              for part in range(3)]
    load_0.append(pltpu.make_async_copy(wo_hbm.at[0], wo0, local_sem.at[4]))
    for copy in load_0:
        copy.start()
    mine = pl.multiple_of(s * half, half)

    def own_w(l):
        base = 5 + 4 * (l - 1)
        copies = [pltpu.make_async_copy(
            wqkv_hbm.at[l, part], wide.at[l - 1, :, pl.ds(part * width + mine, half)], local_sem.at[base + part])
            for part in range(3)]
        copies.append(pltpu.make_async_copy(wo_hbm.at[l], wide_o.at[l - 1, pl.ds(mine, half), :], local_sem.at[base + 3]))
        return copies

    def pass_w(l):
        copies = [pltpu.make_async_remote_copy(
            wqkv_hbm.at[l, part], wide.at[l - 1, :, pl.ds(part * width + mine, half)],
            wsend.at[l - 1, part], wrecv.at[l - 1, part], device_id=partner, device_id_type=MESH)
            for part in range(3)]
        copies.append(pltpu.make_async_remote_copy(
            wo_hbm.at[l], wide_o.at[l - 1, pl.ds(mine, half), :],
            wsend.at[l - 1, 3], wrecv.at[l - 1, 3], device_id=partner, device_id_type=MESH))
        return copies

    for l in (1, 2):
        for copy in own_w(l):
            copy.start()

    i, j = iota((count, count), 0), iota((count, count), 1)
    square = side * side
    turn = one_hot(j == (i // square) * square + lax.rem(i, side) * side + lax.rem(i, square) // side)

    lane = iota((1, PAIR), 1)
    left, right = one_hot(lane < HEAD_DIM), one_hot(lane >= HEAD_DIM)
    r, c2 = iota((tile, tile), 0), iota((tile, tile), 1)
    mean_heads[...] = jnp.where(r // HEAD_DIM == c2 // HEAD_DIM, 1.0 / HEAD_DIM, 0.0).astype(BF16)
    i2, j2 = iota((count, 2 * count), 0), iota((count, 2 * count), 1)
    row_mask[...] = one_hot(lax.rem(i2, band) == lax.rem(j2, band))
    r, c2 = iota((2 * count, PAIR), 0), iota((2 * count, PAIR), 1)
    ones[...] = one_hot(r // count == c2 // HEAD_DIM)

    def span(c):
        return pl.ds(pl.multiple_of(c * band, band), band)

    def normalize(tokens, l):
        values = tokens.astype(F32)
        scale = lax.rsqrt(jnp.mean(values * values, axis=-1, keepdims=True) + EPSILON)
        return (values * scale * gain_ref[l:l + 1, :]).astype(BF16)

    def project(flat, w, total, scaled):
        every, tiles = matmul(flat, w[...]), []
        for start in range(0, total, tile):
            y = every[:, start:min(start + tile, total)]
            if start < scaled:
                y = y * lax.rsqrt(matmul((y * y).astype(BF16), mean_heads[...]) + EPSILON)
            tiles.append(y.astype(BF16))
        return tiles

    def project_tokens(tokens, l, w):
        values = tokens.astype(F32)
        every = matmul((values * gain_ref[l:l + 1, :]).astype(BF16), w[...])
        spread = jnp.mean(values * values, axis=-1, keepdims=True) + EPSILON
        tiles = []
        for start in range(0, 3 * width, tile):
            y = every[:, start:start + tile]
            if start < 2 * width:
                y = y * lax.rsqrt(matmul((y * y).astype(BF16), mean_heads[...]) + EPSILON * spread)
            else:
                y = y * lax.rsqrt(spread)
            tiles.append(y.astype(BF16))
        return tiles

    def pair_of(tiles, p):
        return tiles[p // 2][:, (p % 2) * PAIR:(p % 2 + 1) * PAIR]

    def attend(queries, keys, values, sums, mask):
        scores = [lax.dot_general(q, jnp.concatenate([k * left, k * right], axis=0), CROSS, preferred_element_type=F32)
                  for q, k in zip(queries, keys)]
        expos = [jnp.exp2(score * (math.log2(math.e) / math.sqrt(HEAD_DIM))).astype(BF16) for score in scores]
        if mask is not None:
            expos = [expo * mask for expo in expos]
        outs = []
        for expo, v in zip(expos, values):
            vv = jnp.concatenate([jnp.concatenate([v * left, v * right], axis=0), sums], axis=1)
            both = matmul(expo, vv)
            outs.append((both[:, :PAIR] / both[:, PAIR:]).astype(BF16))
        return jnp.concatenate(outs, axis=1)

    def attention(tiles, n, mask):
        split = [pair_of(tiles, p) for p in range(3 * n)]
        return attend(split[:n], split[n:2 * n], split[2 * n:], ones[...], mask)

    def permute(matrix, values):
        return matmul(matrix, values).astype(BF16)

    def push(src, dst, sem, c, device):
        pltpu.make_async_remote_copy(src, dst, ssem.at[sem, c], rsem.at[sem, c], device_id=device, device_id_type=MESH).start()

    def arrived(ref, sem, c):
        pltpu.make_async_copy(ref, ref, rsem.at[sem, c]).wait()

    def sent(ref, sem, c):
        pltpu.make_async_copy(ref, ref, ssem.at[sem, c]).wait()

    def all_but(ref, c, n):
        return ref.at[c, pl.ds(0, n)]

    def turned(ref, c):
        return permute(turn, ref[c].reshape(count, width)).reshape(2 * side, side, width)

    def start_out(c, values):
        out1[c] = values.reshape(2 * side, side, width)
        for k in order:
            x, y = other(gx, k), other(gy, k)
            push(out1.at[c, x * 2], in1.at[c, gx], 0, c, at_x(x, s))
            push(out1.at[c, y * 2 + 1], in1.at[c, side + gy], 0, c, at_y(y, s))
        in1[c, gx] = out1[c, gx * 2]
        in1[c, side + gy] = out1[c, gy * 2 + 1]

    def relay_out(c):
        arrived(all_but(in1, c, 2 * side - 2), 0, c)
        out2[c] = turned(in1, c)
        for k in order:
            x, y = other(gx, k), other(gy, k)
            push(out2.at[c, y], in2.at[c, gy * 2 + s], 1, c, at_y(y, 0))
            push(out2.at[c, side + x], in2.at[c, gx * 2 + s], 1, c, at_x(x, 1))
        push(out2.at[c, o * side + last_o], in2.at[c, last_o * 2 + s], 1, c, partner)
        in2[c, last * 2 + s] = out2[c, s * side + last]

    def start_back(c, values):
        back1[c] = values.reshape(2 * side, side, width)
        for k in order:
            g = other(last, k)
            chip = s * (g * side + gy) + o * (gx * side + g)
            for core in range(2):
                push(back1.at[c, g * 2 + core], land1.at[c, s * side + last], 2, c, {"tok": chip, "sub": core})
        push(back1.at[c, last * 2 + o], land1.at[c, s * side + last], 2, c, partner)
        land1[c, s * side + last] = back1[c, last * 2 + s]

    def relay_back(c):
        arrived(all_but(land1, c, 2 * side - 1), 2, c)
        back2[c] = turned(land1, c)
        for k in order:
            x, y = other(gx, k), other(gy, k)
            push(back2.at[c, x], x2.at[gx, c, 0], 3, c, at_x(x, s))
            push(back2.at[c, side + y], x2.at[gy, c, 1], 3, c, at_y(y, s))
        x2[gx, c, 0] = back2[c, gx]
        x2[gy, c, 1] = back2[c, side + gy]

    def finish_back(c):
        arrived(all_but(back2, c, 2 * side - 2), 3, c)
        sent(all_but(back2, c, 2 * side - 2), 3, c)

    def pass_normed(c):
        return pltpu.make_async_remote_copy(
            normed.at[0, :, span(c), :], normed.at[1, :, span(c), :], pair_sem.at[0, c], pair_sem.at[1, c],
            device_id=partner, device_id_type=MESH)

    def pass_update(c):
        return pltpu.make_async_remote_copy(
            give.at[:, span(c), :], take.at[:, span(c), :], pair_sem.at[2, c], pair_sem.at[3, c],
            device_id=partner, device_id_type=MESH)

    def project_heads(slot):
        tiles = project(normed[slot].reshape(frames * rows, width), w0, 3 * half, width)
        for part in range(3):
            for p in range(pairs // 2):
                qkv[part, :, :, p * PAIR:(p + 1) * PAIR] = pair_of(tiles, part * (pairs // 2) + p).reshape(frames, rows, PAIR)

    def attend_heads():
        for c in range(chunks):
            at = slice(c * band, (c + 1) * band)
            split = [[qkv[part, :, at, p * PAIR:(p + 1) * PAIR].reshape(count, PAIR) for p in range(pairs // 2)]
                     for part in range(3)]
            mixed[:, at, 0:half] = attend(*split, ones[...], row_mask[...]).reshape(frames, band, half)
        return matmul(mixed[:, :, 0:half].reshape(frames * rows, half), wo0[...])

    load_x.wait()

    @pl.loop(0, chunks)
    def _(c):
        normed[0, :, span(c), :] = normalize(x0[:, span(c), :].reshape(count, width), 0).reshape(frames, band, width)

    for copy in load_0:
        copy.wait()

    project_heads(0)
    pl.semaphore_wait(barrier, 4 * (side - 1) + 1)
    for c in range(chunks):
        pass_normed(c).start()
    own[...] = x0[...].astype(F32) + attend_heads().reshape(frames, rows, width)

    def join(c):
        pass_update(c).wait_recv()
        at = slice(c * band, (c + 1) * band)
        start_out(c, (own[:, at, :] + take[:, at, :].astype(F32)).astype(BF16).reshape(count, width))

    for c in range(chunks):
        pass_normed(c).wait_recv()
        tiles = project(normed[1, :, c * band:(c + 1) * band, :].reshape(count, width), w0, 3 * half, width)
        update = matmul(attention(tiles, pairs // 2, row_mask[...]), wo0[...])
        give[:, c * band:(c + 1) * band, :] = update.astype(BF16).reshape(frames, band, width)
        pass_update(c).start()
        if c > 0:
            join(c - 1)
    join(chunks - 1)

    for copy in pass_w(1):
        copy.start()

    @pl.loop(0, chunks)
    def _(c):
        relay_out(c)

    for copy in pass_w(2):
        copy.start()

    for copy in own_w(1):
        copy.wait()
    for copy in pass_w(1):
        copy.wait_recv()

    @pl.loop(0, chunks)
    def _(c):
        arrived(all_but(in2, c, 2 * side - 1), 1, c)
        line = in2[c].reshape(count, width)
        tiles = project_tokens(line, 1, wide.at[0])
        update = matmul(attention(tiles, pairs, None), wide_o[0])
        start_back(c, (line.astype(F32) + update).astype(BF16))

    @pl.loop(0, chunks)
    def _(c):
        relay_back(c)

    for l in (1, 2):
        for copy in pass_w(l):
            copy.wait_send()

    @pl.loop(0, chunks)
    def _(c):
        pass_normed(c).wait_send()
        pass_update(c).wait_send()
        for sem, (ref, n) in enumerate(((out1, 2), (out2, 1), (back1, 1))):
            sent(all_but(ref, c, 2 * side - n), sem, c)

    def columns(c):
        finish_back(c)
        tiles = project_tokens(x2[:, c].reshape(count, width), 2, wide.at[1])
        for t, value in enumerate(tiles):
            part, at = divmod(t * tile, width)
            qkv[part, :, span(c), at:at + tile] = value.reshape(frames, band, tile)

    for copy in own_w(2):
        copy.wait()
    for copy in pass_w(2):
        copy.wait_recv()

    @pl.loop(0, chunks)
    def _(c):
        columns(c)

    sums = jnp.concatenate([jnp.broadcast_to(left, (rows, PAIR)), jnp.broadcast_to(right, (rows, PAIR))], axis=0)

    lanes = [slice(p * PAIR, (p + 1) * PAIR) for p in range(pairs)]

    @pl.loop(0, frames // 4)
    def _(f4):
        for f in (4 * f4, 4 * f4 + 1, 4 * f4 + 2, 4 * f4 + 3):
            mixed[f] = attend(*([qkv[part, f, :, at] for at in lanes] for part in range(3)), sums, None)

    total = x2[...].reshape(frames * rows, width).astype(F32) + matmul(mixed[...].reshape(frames * rows, width), wide_o[1])
    out_ref[...] = total.astype(BF16).reshape(frames, rows, width)


def body(side, video, norm_gain, qkv_weight, out_weight):
    frames, rows, cols, width = video.shape
    half = width // 2
    lines = 2 * side * side
    chunks = frames * rows // lines
    count = frames * rows // chunks
    blocks = pltpu.VMEM((chunks, 2 * side, side, width), BF16)
    tokens = pltpu.VMEM((frames, rows, width), BF16)
    dma = pltpu.SemaphoreType.DMA
    anywhere = pl.BlockSpec(memory_space=pltpu.HBM)
    vmem = pl.BlockSpec(memory_space=pltpu.VMEM)
    out = pl.pallas_call(
        functools.partial(kernel, side),
        out_shape=jax.ShapeDtypeStruct((frames, rows, width), BF16),
        in_specs=[anywhere, vmem, anywhere, anywhere],
        out_specs=vmem,
        scratch_shapes=[
            tokens,
            pltpu.VMEM((frames, chunks, 2, side, width), BF16),
            pltpu.VMEM((2, frames, rows, width), BF16),
            pltpu.VMEM((3, frames, rows, width), BF16),
            tokens,
            pltpu.VMEM((frames, rows, width), F32), tokens, tokens,
            pltpu.VMEM((width, 3 * half), BF16), pltpu.VMEM((half, width), BF16),
            pltpu.VMEM((2, width, 3 * width), BF16), pltpu.VMEM((2, width, width), BF16),
            pltpu.VMEM((2 * PAIR, 2 * PAIR), BF16), pltpu.VMEM((2 * count, PAIR), BF16),
            pltpu.VMEM((count, 2 * count), BF16),
            blocks, blocks, blocks, blocks, blocks, blocks, blocks,
            dma((13,)), dma((4, chunks)), dma((2, 4)), dma((2, 4)), dma((4, chunks)), dma((4, chunks)),
        ],
        compiler_params=pltpu.CompilerParams(
            collective_id=0, has_side_effects=True, vmem_limit_bytes=50 * 1024 * 1024),
    )(*(pltpu.with_memory_space_constraint(a, pltpu.HBM) for a in (video.reshape(frames, rows, width), norm_gain, qkv_weight, out_weight)))
    return out.reshape(video.shape)


def solution(mesh):
    side = math.isqrt(mesh.shape["tok"])
    in_specs = (
        P("parts", None, ("tok", "sub"), None),
        P(),
        P(None, None, None, "sub"),
        P(None, "sub", None),
    )
    out_specs = P("parts", None, ("tok", "sub"), None)
    return jax.shard_map(functools.partial(body, side), mesh=mesh, in_specs=in_specs, out_specs=out_specs, check_vma=False)
```

```python
import functools
import math

import jax
import jax.numpy as jnp
from jax import lax
from jax.experimental import pallas as pl
from jax.experimental.pallas import tpu as pltpu
from jax.sharding import PartitionSpec as P

HEAD_DIM = 64
EPSILON = 1e-06
PAIR = 2 * HEAD_DIM
MESH = pl.DeviceIdType.MESH
F32, BF16 = jnp.float32, jnp.bfloat16
CROSS = (((1,), (1,)), ((), ()))


def iota(shape, dim):
    return lax.broadcasted_iota(jnp.int32, shape, dim)


def one_hot(condition):
    return jnp.where(condition, 1.0, 0.0).astype(BF16)


def matmul(a, b):
    return jnp.dot(a, b, preferred_element_type=F32)


def kernel(side, video_hbm, gain_hbm, wqkv_hbm, wo_hbm, out_ref, gain_ref,
           x0, x2, normed, qkv, mixed, own, give, take,
           w0, wo0, wide, wide_o, mean_heads, ones, row_mask,
           out1, in1, out2, in2, back1, land1, back2,
           local_sem, pair_sem, wsend, wrecv, ssem, rsem):
    frames, rows, width = x0.shape
    half = width // 2
    pairs = width // PAIR
    chunks = in1.shape[0]
    band = rows // chunks
    count = frames * band
    tile = 2 * PAIR
    tok, s = lax.axis_index("tok"), lax.axis_index("sub")
    o = 1 - s
    gx, gy = tok // side, lax.rem(tok, side)
    last = gx * s + gy * o
    last_o = gx * o + gy * s
    partner = {"sub": o}

    def other(g, k):
        return lax.rem(g + k, side)

    def at_x(g, core):
        return {"tok": g * side + gy, "sub": core}

    def at_y(g, core):
        return {"tok": gx * side + g, "sub": core}

    order = sorted(range(1, side), key=lambda k: -min(k, side - k))
    load_x = pltpu.make_async_copy(video_hbm, x0, local_sem.at[0])
    load_x.start()
    load_gain = pltpu.make_async_copy(gain_hbm, gain_ref, local_sem.at[13])
    load_gain.start()
    barrier = pltpu.get_barrier_semaphore()
    pl.semaphore_signal(barrier, inc=1, device_id=partner, device_id_type=MESH)
    for k in order:
        for core in range(2):
            pl.semaphore_signal(barrier, inc=1, device_id=at_x(other(gx, k), core), device_id_type=MESH)
            pl.semaphore_signal(barrier, inc=1, device_id=at_y(other(gy, k), core), device_id_type=MESH)
    load_0 = [pltpu.make_async_copy(wqkv_hbm.at[0, part], w0.at[:, pl.ds(part * half, half)], local_sem.at[1 + part])
              for part in range(3)]
    load_0.append(pltpu.make_async_copy(wo_hbm.at[0], wo0, local_sem.at[4]))
    for copy in load_0:
        copy.start()
    mine = pl.multiple_of(s * half, half)

    def own_w(l):
        base = 5 + 4 * (l - 1)
        copies = [pltpu.make_async_copy(
            wqkv_hbm.at[l, part], wide.at[l - 1, :, pl.ds(part * width + mine, half)], local_sem.at[base + part])
            for part in range(3)]
        copies.append(pltpu.make_async_copy(wo_hbm.at[l], wide_o.at[l - 1, pl.ds(mine, half), :], local_sem.at[base + 3]))
        return copies

    def pass_w(l):
        copies = [pltpu.make_async_remote_copy(
            wqkv_hbm.at[l, part], wide.at[l - 1, :, pl.ds(part * width + mine, half)],
            wsend.at[l - 1, part], wrecv.at[l - 1, part], device_id=partner, device_id_type=MESH)
            for part in range(3)]
        copies.append(pltpu.make_async_remote_copy(
            wo_hbm.at[l], wide_o.at[l - 1, pl.ds(mine, half), :],
            wsend.at[l - 1, 3], wrecv.at[l - 1, 3], device_id=partner, device_id_type=MESH))
        return copies

    for l in (1, 2):
        for copy in own_w(l):
            copy.start()

    i, j = iota((count, count), 0), iota((count, count), 1)
    square = side * side
    turn = one_hot(j == (i // square) * square + lax.rem(i, side) * side + lax.rem(i, square) // side)

    lane = iota((1, PAIR), 1)
    left, right = one_hot(lane < HEAD_DIM), one_hot(lane >= HEAD_DIM)
    r, c2 = iota((tile, tile), 0), iota((tile, tile), 1)
    mean_heads[...] = jnp.where(r // HEAD_DIM == c2 // HEAD_DIM, 1.0 / HEAD_DIM, 0.0).astype(BF16)
    i2, j2 = iota((count, 2 * count), 0), iota((count, 2 * count), 1)
    row_mask[...] = one_hot(lax.rem(i2, band) == lax.rem(j2, band))
    r, c2 = iota((2 * count, PAIR), 0), iota((2 * count, PAIR), 1)
    ones[...] = one_hot(r // count == c2 // HEAD_DIM)

    def span(c):
        return pl.ds(pl.multiple_of(c * band, band), band)

    def normalize(tokens, l):
        values = tokens.astype(F32)
        scale = lax.rsqrt(jnp.mean(values * values, axis=-1, keepdims=True) + EPSILON)
        return (values * scale * gain_ref[l:l + 1, :]).astype(BF16)

    def project(flat, w, total, scaled):
        every, tiles = matmul(flat, w[...]), []
        for start in range(0, total, tile):
            y = every[:, start:min(start + tile, total)]
            if start < scaled:
                y = y * lax.rsqrt(matmul((y * y).astype(BF16), mean_heads[...]) + EPSILON)
            tiles.append(y.astype(BF16))
        return tiles

    def project_tokens(tokens, l, w):
        values = tokens.astype(F32)
        every = matmul((values * gain_ref[l:l + 1, :]).astype(BF16), w[...])
        spread = jnp.mean(values * values, axis=-1, keepdims=True) + EPSILON
        tiles = []
        for start in range(0, 3 * width, tile):
            y = every[:, start:start + tile]
            if start < 2 * width:
                y = y * lax.rsqrt(matmul((y * y).astype(BF16), mean_heads[...]) + EPSILON * spread)
            else:
                y = y * lax.rsqrt(spread)
            tiles.append(y.astype(BF16))
        return tiles

    def pair_of(tiles, p):
        return tiles[p // 2][:, (p % 2) * PAIR:(p % 2 + 1) * PAIR]

    def attend(queries, keys, values, sums, mask):
        scores = [lax.dot_general(q, jnp.concatenate([k * left, k * right], axis=0), CROSS, preferred_element_type=F32)
                  for q, k in zip(queries, keys)]
        expos = [jnp.exp2(score * (math.log2(math.e) / math.sqrt(HEAD_DIM))).astype(BF16) for score in scores]
        if mask is not None:
            expos = [expo * mask for expo in expos]
        outs = []
        for expo, v in zip(expos, values):
            vv = jnp.concatenate([jnp.concatenate([v * left, v * right], axis=0), sums], axis=1)
            both = matmul(expo, vv)
            outs.append((both[:, :PAIR] / both[:, PAIR:]).astype(BF16))
        return jnp.concatenate(outs, axis=1)

    def attention(tiles, n, mask):
        split = [pair_of(tiles, p) for p in range(3 * n)]
        return attend(split[:n], split[n:2 * n], split[2 * n:], ones[...], mask)

    def permute(matrix, values):
        return matmul(matrix, values).astype(BF16)

    def push(src, dst, sem, c, device):
        pltpu.make_async_remote_copy(src, dst, ssem.at[sem, c], rsem.at[sem, c], device_id=device, device_id_type=MESH).start()

    def arrived(ref, sem, c):
        pltpu.make_async_copy(ref, ref, rsem.at[sem, c]).wait()

    def sent(ref, sem, c):
        pltpu.make_async_copy(ref, ref, ssem.at[sem, c]).wait()

    def all_but(ref, c, n):
        return ref.at[c, pl.ds(0, n)]

    def turned(ref, c):
        return permute(turn, ref[c].reshape(count, width)).reshape(2 * side, side, width)

    def start_out(c, values):
        out1[c] = values.reshape(2 * side, side, width)
        for k in order:
            x, y = other(gx, k), other(gy, k)
            push(out1.at[c, x * 2], in1.at[c, gx], 0, c, at_x(x, s))
            push(out1.at[c, y * 2 + 1], in1.at[c, side + gy], 0, c, at_y(y, s))
        in1[c, gx] = out1[c, gx * 2]
        in1[c, side + gy] = out1[c, gy * 2 + 1]

    def relay_out(c):
        arrived(all_but(in1, c, 2 * side - 2), 0, c)
        out2[c] = turned(in1, c)
        for k in order:
            x, y = other(gx, k), other(gy, k)
            push(out2.at[c, y], in2.at[c, gy * 2 + s], 1, c, at_y(y, 0))
            push(out2.at[c, side + x], in2.at[c, gx * 2 + s], 1, c, at_x(x, 1))
        push(out2.at[c, o * side + last_o], in2.at[c, last_o * 2 + s], 1, c, partner)
        in2[c, last * 2 + s] = out2[c, s * side + last]

    def start_back(c, values):
        back1[c] = values.reshape(2 * side, side, width)
        for k in order:
            g = other(last, k)
            chip = s * (g * side + gy) + o * (gx * side + g)
            for core in range(2):
                push(back1.at[c, g * 2 + core], land1.at[c, s * side + last], 2, c, {"tok": chip, "sub": core})
        push(back1.at[c, last * 2 + o], land1.at[c, s * side + last], 2, c, partner)
        land1[c, s * side + last] = back1[c, last * 2 + s]

    def relay_back(c):
        arrived(all_but(land1, c, 2 * side - 1), 2, c)
        back2[c] = turned(land1, c)
        for k in order:
            x, y = other(gx, k), other(gy, k)
            push(back2.at[c, x], x2.at[gx, c, 0], 3, c, at_x(x, s))
            push(back2.at[c, side + y], x2.at[gy, c, 1], 3, c, at_y(y, s))
        x2[gx, c, 0] = back2[c, gx]
        x2[gy, c, 1] = back2[c, side + gy]

    def finish_back(c):
        arrived(all_but(back2, c, 2 * side - 2), 3, c)
        sent(all_but(back2, c, 2 * side - 2), 3, c)

    def pass_normed(c):
        return pltpu.make_async_remote_copy(
            normed.at[0, :, span(c), :], normed.at[1, :, span(c), :], pair_sem.at[0, c], pair_sem.at[1, c],
            device_id=partner, device_id_type=MESH)

    def pass_update(c):
        return pltpu.make_async_remote_copy(
            give.at[:, span(c), :], take.at[:, span(c), :], pair_sem.at[2, c], pair_sem.at[3, c],
            device_id=partner, device_id_type=MESH)

    def project_heads(slot):
        tiles = project(normed[slot].reshape(frames * rows, width), w0, 3 * half, width)
        for part in range(3):
            for p in range(pairs // 2):
                qkv[part, :, :, p * PAIR:(p + 1) * PAIR] = pair_of(tiles, part * (pairs // 2) + p).reshape(frames, rows, PAIR)

    def attend_heads():
        for c in range(chunks):
            at = slice(c * band, (c + 1) * band)
            split = [[qkv[part, :, at, p * PAIR:(p + 1) * PAIR].reshape(count, PAIR) for p in range(pairs // 2)]
                     for part in range(3)]
            mixed[:, at, 0:half] = attend(*split, ones[...], row_mask[...]).reshape(frames, band, half)
        return matmul(mixed[:, :, 0:half].reshape(frames * rows, half), wo0[...])

    load_x.wait()
    load_gain.wait()

    @pl.loop(0, chunks)
    def _(c):
        normed[0, :, span(c), :] = normalize(x0[:, span(c), :].reshape(count, width), 0).reshape(frames, band, width)

    for copy in load_0:
        copy.wait()

    project_heads(0)
    pl.semaphore_wait(barrier, 4 * (side - 1) + 1)
    for c in range(chunks):
        pass_normed(c).start()
    own[...] = x0[...].astype(F32) + attend_heads().reshape(frames, rows, width)

    def join(c):
        pass_update(c).wait_recv()
        at = slice(c * band, (c + 1) * band)
        start_out(c, (own[:, at, :] + take[:, at, :].astype(F32)).astype(BF16).reshape(count, width))

    for c in range(chunks):
        pass_normed(c).wait_recv()
        tiles = project(normed[1, :, c * band:(c + 1) * band, :].reshape(count, width), w0, 3 * half, width)
        update = matmul(attention(tiles, pairs // 2, row_mask[...]), wo0[...])
        give[:, c * band:(c + 1) * band, :] = update.astype(BF16).reshape(frames, band, width)
        pass_update(c).start()
        if c > 0:
            join(c - 1)
    join(chunks - 1)

    for copy in pass_w(1):
        copy.start()

    @pl.loop(0, chunks)
    def _(c):
        relay_out(c)

    for copy in pass_w(2):
        copy.start()

    for copy in own_w(1):
        copy.wait()
    for copy in pass_w(1):
        copy.wait_recv()

    @pl.loop(0, chunks)
    def _(c):
        arrived(all_but(in2, c, 2 * side - 1), 1, c)
        line = in2[c].reshape(count, width)
        tiles = project_tokens(line, 1, wide.at[0])
        update = matmul(attention(tiles, pairs, None), wide_o[0])
        start_back(c, (line.astype(F32) + update).astype(BF16))

    @pl.loop(0, chunks)
    def _(c):
        relay_back(c)

    for l in (1, 2):
        for copy in pass_w(l):
            copy.wait_send()

    @pl.loop(0, chunks)
    def _(c):
        pass_normed(c).wait_send()
        pass_update(c).wait_send()
        for sem, (ref, n) in enumerate(((out1, 2), (out2, 1), (back1, 1))):
            sent(all_but(ref, c, 2 * side - n), sem, c)

    def columns(c):
        finish_back(c)
        tiles = project_tokens(x2[:, c].reshape(count, width), 2, wide.at[1])
        for t, value in enumerate(tiles):
            part, at = divmod(t * tile, width)
            qkv[part, :, span(c), at:at + tile] = value.reshape(frames, band, tile)

    for copy in own_w(2):
        copy.wait()
    for copy in pass_w(2):
        copy.wait_recv()

    @pl.loop(0, chunks)
    def _(c):
        columns(c)

    sums = jnp.concatenate([jnp.broadcast_to(left, (rows, PAIR)), jnp.broadcast_to(right, (rows, PAIR))], axis=0)

    lanes = [slice(p * PAIR, (p + 1) * PAIR) for p in range(pairs)]

    @pl.loop(0, frames // 4)
    def _(f4):
        for f in (4 * f4, 4 * f4 + 1, 4 * f4 + 2, 4 * f4 + 3):
            mixed[f] = attend(*([qkv[part, f, :, at] for at in lanes] for part in range(3)), sums, None)

    total = x2[...].reshape(frames * rows, width).astype(F32) + matmul(mixed[...].reshape(frames * rows, width), wide_o[1])
    out_ref[...] = total.astype(BF16).reshape(frames, rows, width)


def body(side, video, norm_gain, qkv_weight, out_weight):
    frames, rows, cols, width = video.shape
    half = width // 2
    lines = 2 * side * side
    chunks = frames * rows // lines
    count = frames * rows // chunks
    blocks = pltpu.VMEM((chunks, 2 * side, side, width), BF16)
    tokens = pltpu.VMEM((frames, rows, width), BF16)
    dma = pltpu.SemaphoreType.DMA
    anywhere = pl.BlockSpec(memory_space=pltpu.HBM)
    vmem = pl.BlockSpec(memory_space=pltpu.VMEM)
    out = pl.pallas_call(
        functools.partial(kernel, side),
        out_shape=jax.ShapeDtypeStruct((frames, rows, width), BF16),
        in_specs=[anywhere, anywhere, anywhere, anywhere],
        out_specs=vmem,
        scratch_shapes=[
            pltpu.VMEM(norm_gain.shape, F32),
            tokens,
            pltpu.VMEM((frames, chunks, 2, side, width), BF16),
            pltpu.VMEM((2, frames, rows, width), BF16),
            pltpu.VMEM((3, frames, rows, width), BF16),
            tokens,
            pltpu.VMEM((frames, rows, width), F32), tokens, tokens,
            pltpu.VMEM((width, 3 * half), BF16), pltpu.VMEM((half, width), BF16),
            pltpu.VMEM((2, width, 3 * width), BF16), pltpu.VMEM((2, width, width), BF16),
            pltpu.VMEM((2 * PAIR, 2 * PAIR), BF16), pltpu.VMEM((2 * count, PAIR), BF16),
            pltpu.VMEM((count, 2 * count), BF16),
            blocks, blocks, blocks, blocks, blocks, blocks, blocks,
            dma((14,)), dma((4, chunks)), dma((2, 4)), dma((2, 4)), dma((4, chunks)), dma((4, chunks)),
        ],
        compiler_params=pltpu.CompilerParams(
            collective_id=0, has_side_effects=True, vmem_limit_bytes=50 * 1024 * 1024),
    )(*(pltpu.with_memory_space_constraint(a, pltpu.HBM) for a in (video.reshape(frames, rows, width), norm_gain, qkv_weight, out_weight)))
    return out.reshape(video.shape)


def solution(mesh):
    side = math.isqrt(mesh.shape["tok"])
    in_specs = (
        P("parts", None, ("tok", "sub"), None),
        P(),
        P(None, None, None, "sub"),
        P(None, "sub", None),
    )
    out_specs = P("parts", None, ("tok", "sub"), None)
    return jax.shard_map(functools.partial(body, side), mesh=mesh, in_specs=in_specs, out_specs=out_specs, check_vma=False)
```
